32 devices in a mesh: cells: 8 (over z, y), bins: 4 (over x, core).
Axes of the slice: x: 2, y: 2, z: 4, core: 2. Of those that a mesh axis runs over, the one named last changes fastest.
Arguments:
- snapshots: bfloat16 [4, 65536, 512], P('bins', 'cells'), may hold values from -150 to 150
- training: int32 [65536], P('cells'), may hold values 0 or 1
- doppler: int32 [4, 128], P('bins'), may hold values from 0 to 1023
Outputs:
- filtered: bfloat16 [4, 256, 65536], P('bins', None, 'cells')
The draws below stay inside these ranges and needn't reach their ends.
All inputs are finite; a program needn't handle non-finite values. No bound on the sum of `training` on one device may be relied on, other than what follows from the above.
Results may differ from the reference program's by a relative error of at most 0.003.
The reference program's roundings to bfloat16 on the way (of `taps`) count: a program that leaves them out, or rounds other values in their place, can miss the bound.
Values sent between devices are 32-bit elements; how exact they have to be, the bound alone decides.
A program may use at most 64 MiB of HBM per device.

```python
import jax
import jax.numpy as jnp
from jax import lax

CHANNELS = 16
PULSES = 16
DIM = 256
BINS_G = 128
NDOPP = 1024
CELLS = 65536
GROUPS = 4


def draw_snapshots(key, part):
    keys = jax.random.split(jax.random.fold_in(key, 7101), 13)
    patches = CHANNELS + PULSES
    jammers = 2
    width = 2 * DIM
    noise_part = jnp.clip(jax.random.normal(keys[0], (GROUPS, CELLS, width), jnp.float32), -4.0, 4.0)
    clutter_re = jnp.clip(jax.random.normal(keys[1], (GROUPS, CELLS, patches), jnp.float32), -4.0, 4.0) * 0.7071
    clutter_im = jnp.clip(jax.random.normal(keys[2], (GROUPS, CELLS, patches), jnp.float32), -4.0, 4.0) * 0.7071
    jam_re = jnp.clip(jax.random.normal(keys[3], (GROUPS, CELLS, jammers, PULSES), jnp.float32), -4.0, 4.0) * 0.7071
    jam_im = jnp.clip(jax.random.normal(keys[4], (GROUPS, CELLS, jammers, PULSES), jnp.float32), -4.0, 4.0) * 0.7071
    gains = jnp.exp(jax.random.uniform(keys[5], (GROUPS, 1, DIM), jnp.float32, jnp.log(0.5), jnp.log(2.0)))
    index = jnp.arange(DIM)
    chan = (index // PULSES).astype(jnp.float32)
    pulse = (index % PULSES).astype(jnp.float32)
    offset = jax.random.uniform(keys[6], (GROUPS, 1), jnp.float32, 0.0, 1.0)
    spatial = (jnp.arange(patches).astype(jnp.float32)[None, :] + offset) / patches - 0.5
    slope = jax.random.uniform(keys[7], (GROUPS, 1), jnp.float32, 0.8, 1.2)
    temporal = slope * spatial
    phase = 2.0 * jnp.pi * (spatial[:, :, None] * chan[None, None, :] + temporal[:, :, None] * pulse[None, None, :])
    patch_power = jnp.exp(jax.random.uniform(keys[8], (GROUPS, 1, patches), jnp.float32, jnp.log(0.5), jnp.log(8.0)))
    amp_re = clutter_re * jnp.sqrt(patch_power)
    amp_im = clutter_im * jnp.sqrt(patch_power)
    cosines = jnp.cos(phase)
    sines = jnp.sin(phase)
    real_sum = jnp.einsum('gnk,gkd->gnd', amp_re, cosines) - jnp.einsum('gnk,gkd->gnd', amp_im, sines)
    imag_sum = jnp.einsum('gnk,gkd->gnd', amp_re, sines) + jnp.einsum('gnk,gkd->gnd', amp_im, cosines)
    jam_angle = jax.random.uniform(keys[9], (GROUPS, jammers), jnp.float32, -0.5, 0.5)
    jam_power = jnp.exp(jax.random.uniform(keys[10], (GROUPS, 1, jammers, 1), jnp.float32, jnp.log(10.0), jnp.log(60.0)))
    chans = jnp.arange(CHANNELS).astype(jnp.float32)
    jam_phase = 2.0 * jnp.pi * jam_angle[:, :, None] * chans[None, None, :]
    jam_cos = jnp.cos(jam_phase)
    jam_sin = jnp.sin(jam_phase)
    jr = jam_re * jnp.sqrt(jam_power)
    ji = jam_im * jnp.sqrt(jam_power)
    jam_real = jnp.einsum('gnjp,gjc->gncp', jr, jam_cos) - jnp.einsum('gnjp,gjc->gncp', ji, jam_sin)
    jam_imag = jnp.einsum('gnjp,gjc->gncp', jr, jam_sin) + jnp.einsum('gnjp,gjc->gncp', ji, jam_cos)
    real_sum = real_sum + jam_real.reshape(GROUPS, CELLS, DIM)
    imag_sum = imag_sum + jam_imag.reshape(GROUPS, CELLS, DIM)
    signal = jnp.concatenate([real_sum, imag_sum], -1) + noise_part
    both_gains = jnp.concatenate([gains, gains], -1)
    rough = jnp.exp(jax.random.uniform(keys[11], (GROUPS, CELLS, 1), jnp.float32, 0.0, jnp.log(3.0)))
    place = jnp.arange(CELLS).astype(jnp.float32) / CELLS
    ranged = (0.6 + 1.4 * place)[None, :, None]
    order = jax.random.permutation(keys[12], GROUPS).astype(jnp.float32)
    level = (1.0 + 2.0 * order / max(GROUPS - 1, 1))[:, None, None]
    return jnp.clip(0.15 * signal * both_gains * rough * ranged * level, -150.0, 150.0).astype(jnp.bfloat16)


def plant(array, key, low, top_value):
    longest = array.shape.index(max(array.shape))
    spots = []
    for shift in (0, 1):
        where = [jax.random.randint(jax.random.fold_in(key, axis), (), 0, length) for axis, length in enumerate(array.shape)]
        where[longest] = (where[longest] + shift) % array.shape[longest]
        spots.append(tuple(where))
    return array.at[spots[0]].set(low).at[spots[1]].set(top_value)


def setup_inputs(seed: int = 0) -> dict:
    seeds = jax.random.split(jax.random.key(seed), 4)
    snapshots = draw_snapshots(jax.random.fold_in(seeds[3], 71), 0)
    training = plant((jax.random.randint(seeds[1], (CELLS,), 0, 4) < 3).astype(jnp.int32), jax.random.fold_in(seeds[1], 1), 0, 1)
    doppler = plant(jax.random.randint(seeds[2], (GROUPS, BINS_G), 0, NDOPP), jax.random.fold_in(seeds[2], 1), 0, NDOPP - 1).astype(jnp.int32)
    return {"snapshots": snapshots, "training": training, "doppler": doppler}


load_ratio = 0.5
look_freq = 0.125

def steering(doppler):
    index = jnp.arange(CHANNELS * PULSES)
    chan = (index // PULSES).astype(jnp.float32)
    pulse = (index % PULSES).astype(jnp.float32)
    freq = doppler.astype(jnp.float32) / NDOPP - 0.5
    phase = 2.0 * jnp.pi * (look_freq * chan[:, None] + pulse[:, None] * freq[None, :])
    return jnp.concatenate([jnp.cos(phase), jnp.sin(phase)], 0) / jnp.sqrt(jnp.float32(DIM))

def complex_parts(gram):
    half = gram.shape[0] // 2
    upper = gram[:half, :half]
    cross = gram[:half, half:]
    lower = gram[half:, half:]
    return (upper + lower, cross.T - cross)

def filter_group(real_part, imag_part, noise, doppler, snaps):
    half = real_part.shape[0]
    loaded = real_part + load_ratio * noise * jnp.eye(half, dtype=jnp.float32)
    embed = jnp.concatenate([jnp.concatenate([loaded, -imag_part], 1), jnp.concatenate([imag_part, loaded], 1)], 0)
    factor = jnp.linalg.cholesky(embed)
    steer = steering(doppler)
    weights = jax.scipy.linalg.cho_solve((factor, True), steer)
    gain = lax.optimization_barrier(jnp.sum(steer * weights, axis=0))
    w_real = weights[:half] / gain[None, :]
    w_imag = weights[half:] / gain[None, :]
    taps = jnp.concatenate([jnp.concatenate([w_real, w_imag], 0), jnp.concatenate([-w_imag, w_real], 0)], 1).astype(jnp.bfloat16)
    result = lax.dot_general(taps.astype(jnp.float32), snaps.astype(jnp.float32), (((0,), (1,)), ((), ())), preferred_element_type=jnp.float32)
    return result.astype(jnp.bfloat16)

def reference(snapshots, training, doppler):
    keep = training.astype(jnp.bfloat16)[:, None]
    parts = []
    power = jnp.float32(0.0)
    for group in range(GROUPS):
        snaps = snapshots[group]
        gram = lax.dot_general((snaps * keep).astype(jnp.float32), snaps.astype(jnp.float32), (((0,), (0,)), ((), ())), preferred_element_type=jnp.float32)
        real_part, imag_part = complex_parts(gram)
        parts.append((real_part, imag_part))
        power = power + jnp.trace(real_part)
    noise = power / (GROUPS * DIM)
    outputs = []
    for group in range(GROUPS):
        outputs.append(filter_group(parts[group][0], parts[group][1], noise, doppler[group], snapshots[group]))
    return jnp.stack(outputs)
```

```python
import functools
import math

import jax
import jax.numpy as jnp
from jax import lax
from jax.experimental import pallas as pl
from jax.experimental.pallas import tpu as pltpu
from jax.sharding import PartitionSpec as P

CHANNELS = 16
PULSES = 16
NDOPP = 1024


load_ratio = 0.5
look_freq = 0.125

EXTRA = 8
HIGH = lax.Precision.HIGH
MESH = pl.DeviceIdType.MESH


def gram_kernel(half, x_ref, keep_ref, out_ref, real_sum, cross_sum):
    step = pl.program_id(0)

    @pl.when(step == 0)
    def _():
        real_sum[...] = jnp.zeros_like(real_sum)
        cross_sum[...] = jnp.zeros_like(cross_sum)

    x = x_ref[...]
    keep = keep_ref[...].astype(jnp.bfloat16)
    masked = x.T * keep
    mr, mi = masked[:half], masked[half:]
    r, i = x[:, :half], x[:, half:]
    real_sum[...] += jnp.dot(
        jnp.concatenate([mr, mi], 1),
        jnp.concatenate([r, i], 0),
        preferred_element_type=jnp.float32,
    )
    cross_sum[...] += jnp.dot(mr, i, preferred_element_type=jnp.float32)

    @pl.when(step == pl.num_programs(0) - 1)
    def _():
        real = real_sum[...]
        cross = cross_sum[...]
        rows = lax.broadcasted_iota(jnp.int32, (half, half), 0)
        cols = lax.broadcasted_iota(jnp.int32, (half, half), 1)
        out_ref[...] = jnp.where(rows <= cols, real, cross.T - cross)


def gram(snaps, keep, block):
    cells, width = snaps.shape
    half = width // 2
    return pl.pallas_call(
        functools.partial(gram_kernel, half),
        grid=(cells // block,),
        in_specs=[
            pl.BlockSpec((block, width), lambda i: (i, 0)),
            pl.BlockSpec((1, block), lambda i: (0, i)),
        ],
        out_specs=pl.BlockSpec((half, half), lambda i: (0, 0)),
        out_shape=jax.ShapeDtypeStruct((half, half), jnp.float32),
        scratch_shapes=[
            pltpu.VMEM((half, half), jnp.float32),
            pltpu.VMEM((half, half), jnp.float32),
        ],
        name="gram",
    )(snaps, keep)


def sum_kernel(n, m, x_ref, out_ref, rs_buf, tr_src, tr_buf, mine, sems):
    me = lax.axis_index("cells")
    g = lax.axis_index("bins")
    half = x_ref.shape[0]
    rows = half // n
    rs_send, rs_recv, tr_send, tr_recv, ag_send, ag_recv = sems

    barrier = pltpu.get_barrier_semaphore()
    for k in range(1, n):
        pl.semaphore_signal(
            barrier, inc=1, device_id=(lax.rem(me + k, n), g), device_id_type=MESH
        )
    for k in range(1, m):
        pl.semaphore_signal(
            barrier, inc=1, device_id=(me, lax.rem(g + k, m)), device_id_type=MESH
        )
    pl.semaphore_wait(barrier, n + m - 2)

    copies = []
    for k in range(1, n):
        peer = lax.rem(me + k, n)
        copy = pltpu.make_async_remote_copy(
            src_ref=x_ref.at[pl.ds(pl.multiple_of(peer * rows, rows), rows)],
            dst_ref=rs_buf.at[k - 1],
            send_sem=rs_send.at[k - 1],
            recv_sem=rs_recv.at[k - 1],
            device_id=(peer, g),
            device_id_type=MESH,
        )
        copy.start()
        copies.append(copy)
    r = lax.broadcasted_iota(jnp.int32, (half, half), 0)
    c = lax.broadcasted_iota(jnp.int32, (half, half), 1)
    trace = jnp.sum(jnp.where(r == c, x_ref[...], 0.0), axis=0, keepdims=True)
    tr_src[...] = jnp.broadcast_to(trace, tr_src.shape)
    for k in range(1, m):
        copy = pltpu.make_async_remote_copy(
            src_ref=tr_src,
            dst_ref=tr_buf.at[k - 1],
            send_sem=tr_send.at[k - 1],
            recv_sem=tr_recv.at[k - 1],
            device_id=(me, lax.rem(g + k, m)),
            device_id_type=MESH,
        )
        copy.start()
        copies.append(copy)
    for copy in copies:
        copy.wait()
    total = x_ref[pl.ds(pl.multiple_of(me * rows, rows), rows), :]
    for k in range(n - 1):
        total = total + rs_buf[k]
    power = tr_src[...]
    for k in range(m - 1):
        power = power + tr_buf[k]
    mine[pl.ds(0, rows), :] = total
    mine[pl.ds(rows, EXTRA), :] = power
    out_ref[me] = jnp.concatenate([total, power], 0)

    copies = []
    for k in range(1, n):
        copy = pltpu.make_async_remote_copy(
            src_ref=mine,
            dst_ref=out_ref.at[me],
            send_sem=ag_send.at[k - 1],
            recv_sem=ag_recv.at[k - 1],
            device_id=(lax.rem(me + k, n), g),
            device_id_type=MESH,
        )
        copy.start()
        copies.append(copy)
    for k in range(1, n):
        copies[k - 1].wait_send()
        pltpu.make_async_remote_copy(
            src_ref=mine,
            dst_ref=out_ref.at[lax.rem(me + n - k, n)],
            send_sem=ag_send.at[k - 1],
            recv_sem=ag_recv.at[k - 1],
            device_id=(lax.rem(me + n - k, n), g),
            device_id_type=MESH,
        ).wait_recv()


def all_sum(packed):
    n, m = lax.axis_size("cells"), lax.axis_size("bins")
    half = packed.shape[0]
    rows = half // n
    dma = pltpu.SemaphoreType.DMA
    return pl.pallas_call(
        functools.partial(sum_kernel, n, m),
        out_shape=jax.ShapeDtypeStruct((n, rows + EXTRA, half), jnp.float32),
        in_specs=[pl.BlockSpec(memory_space=pltpu.VMEM)],
        out_specs=pl.BlockSpec(memory_space=pltpu.VMEM),
        scratch_shapes=[
            pltpu.VMEM((n - 1, rows, half), jnp.float32),
            pltpu.VMEM((EXTRA, half), jnp.float32),
            pltpu.VMEM((m - 1, EXTRA, half), jnp.float32),
            pltpu.VMEM((rows + EXTRA, half), jnp.float32),
            [dma((n - 1,)), dma((n - 1,)), dma((m - 1,)), dma((m - 1,)), dma((n - 1,)), dma((n - 1,))],
        ],
        compiler_params=pltpu.CompilerParams(collective_id=0, has_side_effects=True),
        name="all_sum",
    )(packed)


def grow(d):
    return (4.0 * d - 2.0 * d * d) / (1.0 + 2.0 * d - d * d)


def start_for(steps, goal):
    lo, hi = 0.0, 1.0
    for _ in range(100):
        mid = 0.5 * (lo + hi)
        d = mid
        for _ in range(steps):
            d = grow(d)
        lo, hi = (lo, mid) if d >= goal else (mid, hi)
    return hi


def split(x, parts):
    out = []
    for _ in range(parts):
        top = x.astype(jnp.bfloat16)
        out.append(top)
        x = x - top.astype(jnp.float32)
    return out


def mxu(a, b):
    return jnp.dot(a, b, preferred_element_type=jnp.float32)


def total(x):
    return jnp.sum(jnp.sum(x, axis=0, keepdims=True), axis=1, keepdims=True)


def steer_rows(doppler, chans, pulses):
    bins, dim = doppler.shape[0], chans * pulses
    index = lax.broadcasted_iota(jnp.int32, (1, dim), 1)
    pulse = lax.rem(index, pulses)
    chan = ((index - pulse) // pulses).astype(jnp.float32)
    freq = doppler.astype(jnp.float32) * (1.0 / NDOPP) - 0.5
    turns = look_freq * chan + pulse.astype(jnp.float32) * freq
    phase = (2.0 * math.pi) * turns
    quarter = jnp.floor(4.0 * turns + 0.5)
    rest = phase - quarter * 1.5703125
    rest = rest - quarter * 4.837512969970703125e-4
    rest = rest - quarter * 7.549789948768648e-8
    sq = rest * rest
    sin = rest + rest * sq * (
        -1.6666654611e-1 + sq * (8.3321608736e-3 + sq * -1.9515295891e-4)
    )
    cos = 1.0 + sq * (
        -0.5 + sq * (4.166664568298827e-2 + sq * (-1.388731625493765e-3 + sq * 2.443315711809948e-5))
    )
    which = quarter.astype(jnp.int32) & 3
    odd = (which & 1) == 1
    c = jnp.where(odd, sin, cos)
    s = jnp.where(odd, cos, sin)
    c = jnp.where((which == 1) | (which == 2), -c, c)
    s = jnp.where(which >= 2, -s, s)
    return jnp.concatenate([c, s], 1) * (1.0 / math.sqrt(dim))


def solve_kernel(
    groups, block, parts_ref, dop_ref, x_hbm, out_hbm,
    x_buf, out_buf, taps, e0, e1, e2, low_mat, low_pair, pair, xs, ys, acol, steer, w_ref, in_sems, out_sems,
):
    n = parts_ref.shape[0]
    rows = parts_ref.shape[1] - EXTRA
    half = parts_ref.shape[2]
    full = 2 * half
    bins = dop_ref.shape[0]
    cells = x_buf.shape[0]
    f32, bf16 = jnp.float32, jnp.bfloat16

    loads = []
    for k in range(cells // block):
        span = pl.ds(k * block, block)
        copy = pltpu.make_async_copy(x_hbm.at[span], x_buf.at[span], in_sems.at[k])
        copy.start()
        loads.append(copy)

    summed = jnp.concatenate([parts_ref[k, :rows, :] for k in range(n)], 0)
    power_row = parts_ref[0, rows:rows + 1, :]
    for k in range(1, n):
        power_row = power_row + parts_ref[k, rows:rows + 1, :]
    noise = jnp.sum(power_row, axis=1, keepdims=True) / (groups * half)
    low = load_ratio * noise
    r = lax.broadcasted_iota(jnp.int32, (half, half), 0)
    c = lax.broadcasted_iota(jnp.int32, (half, half), 1)
    diag = jnp.where(r == c, summed, 0.0)
    trace = total(diag)
    unit = 1.0 / (trace + low)
    norm = summed * unit
    fro = jnp.sqrt(total(2.0 * norm * norm - jnp.where(r == c, norm * norm, 0.0))) * (trace + low)
    bound = jnp.minimum(trace, 1.0001 * fro)
    scale = 2.0 / (bound + 2.0 * low)
    eye = jnp.where(r == c, 1.0, 0.0)
    flip = summed.T
    real = (jnp.where(r <= c, summed, flip) + low * eye) * scale
    imag = jnp.where(r > c, summed, jnp.where(r < c, -flip, 0.0)) * scale
    acol[:half, :] = real
    acol[half:, :] = imag

    def quads(ref, base, xr, xi):
        ref[pl.ds(base, half), :half] = xr
        ref[pl.ds(base + half, half), half:] = xr
        ref[pl.ds(base, half), half:] = -xi
        ref[pl.ds(base + half, half), :half] = xi

    for ref, xr, xi in zip((e0, e1, e2), split(real, 3), split(imag, 3)):
        quads(ref, 0, xr, xi)
    steer[...] = steer_rows(dop_ref[...], CHANNELS, PULSES)

    square = mxu(e0[...], e0[:, :half])
    top = total(square * square)
    lam = 1.005 * jnp.sqrt(jnp.sqrt(top)) / scale - low
    tight = jnp.minimum(bound, jnp.maximum(lam, 0.0))
    gainup = (bound + 2.0 * low) / (tight + 2.0 * low)
    d0 = 2.0 * low / (tight + 2.0 * low)

    def first(square, d):
        bend = 2.0 / (1.0 + 2.0 * d - d * d)
        a = acol[...] * gainup
        eyes = jnp.concatenate([eye, jnp.zeros_like(eye)], 0)
        xs[...] = bend * (2.0 * eyes - a)
        ys[...] = bend * (2.0 * a - square * (gainup * gainup))
        return grow(d)

    def steps_of(d):
        count = jnp.zeros_like(d)
        for k in range(2, 12):
            count = count + jnp.where(d < START[k], 1.0, 0.0)
        return jnp.max(count).astype(jnp.int32)

    coarse = jnp.max(jnp.where(d0 < COARSE, 1.0, 0.0)) > 0.5

    @pl.when(jnp.logical_not(coarse))
    def _():
        d1 = first(square, d0)

        def pack(which):
            v = xs if which == 0 else ys
            quads(pair, which * full, v[:half, :].astype(bf16), v[half:, :].astype(bf16))

        pack(0)
        pack(1)

        def body(_, d):
            bend = 2.0 / (1.0 + 2.0 * d - d * d)
            prod = mxu(pair[...], pair[full:, :half])
            xs[...] = bend * (2.0 * xs[...] - prod[:full])
            ys[...] = bend * (2.0 * ys[...] - prod[full:])
            pack(0)
            pack(1)
            return grow(d)

        d = lax.fori_loop(0, steps_of(d0), body, d1)
        bend = 2.0 / (1.0 + 2.0 * d - d * d)
        xs[...] = bend * (2.0 * xs[...] - mxu(pair[:full, :], pair[full:, :half]))
        pack(0)

    @pl.when(coarse)
    def _():
        quads(low_mat, 0, acol[:half, :], acol[half:, :])
        exact = jnp.dot(low_mat[...], acol[...], preferred_element_type=f32, precision=HIGH)
        d1 = first(exact, d0)

        def body(_, d):
            bend = 2.0 / (1.0 + 2.0 * d - d * d)
            quads(low_pair, 0, xs[:half, :], xs[half:, :])
            quads(low_pair, full, ys[:half, :], ys[half:, :])
            prod = jnp.dot(low_pair[...], ys[...], preferred_element_type=f32, precision=HIGH)
            xs[...] = bend * (2.0 * xs[...] - prod[:full])
            ys[...] = bend * (2.0 * ys[...] - prod[full:])
            return grow(d)

        lax.fori_loop(0, steps_of(d0) + 1, body, d1)
        quads(pair, 0, xs[:half, :].astype(bf16), xs[half:, :].astype(bf16))

    def refine(w, passes):
        parts = split(w, passes)
        gap = mxu(jnp.concatenate(parts, 0), e0[...])
        if passes == 3:
            mid = mxu(jnp.concatenate(parts[:2], 0), e1[...])
            tail = mxu(parts[0], e2[...])
            fine = (gap[2 * bins:] + mid[bins:] + tail) + (gap[bins:2 * bins] + mid[:bins])
        else:
            fine = gap[bins:] + mxu(parts[0], e1[...])
        rest = (steer[...] - gap[:bins]) - fine
        return w + mxu(rest.astype(bf16), pair[:full, :]) * gainup

    w = mxu(steer[...].astype(bf16), pair[:full, :]) * gainup
    w = refine(w, 2)
    w_ref[...] = refine(w, 2)

    @pl.when(coarse)
    def _():
        def body(_, w):
            return refine(w, 3)
        w_ref[...] = lax.fori_loop(0, 3, body, w_ref[...])

    w = refine(w_ref[...], 3)
    gain = jnp.sum(steer[...] * w, axis=1, keepdims=True)
    w = w / gain
    wr, wi = w[:, :half], w[:, half:]
    taps[:bins, :half] = wr.astype(bf16)
    taps[:bins, half:] = wi.astype(bf16)
    taps[bins:, :half] = (-wi).astype(bf16)
    taps[bins:, half:] = wr.astype(bf16)

    for copy in loads:
        copy.wait()
    stores = []
    for k in range(cells // block):
        span = pl.ds(k * block, block)
        out_buf[:, span] = lax.dot_general(
            taps[...], x_buf[span, :], (((1,), (1,)), ((), ())), preferred_element_type=f32
        ).astype(bf16)
        copy = pltpu.make_async_copy(out_buf.at[:, span], out_hbm.at[:, span], out_sems.at[k])
        copy.start()
        stores.append(copy)
    for copy in stores:
        copy.wait()


GOAL = 0.95
START = [start_for(k, GOAL) for k in range(12)]
COARSE = 0.005


def solve(parts, doppler, snaps, groups, block):
    half = parts.shape[2]
    bins = doppler.shape[0]
    cells, width = snaps.shape
    full = 2 * half
    f32, bf16 = jnp.float32, jnp.bfloat16
    vmem = pltpu.VMEM
    dma = pltpu.SemaphoreType.DMA
    return pl.pallas_call(
        functools.partial(solve_kernel, groups, block),
        out_shape=jax.ShapeDtypeStruct((2 * bins, cells), bf16),
        in_specs=[
            pl.BlockSpec(memory_space=pltpu.VMEM),
            pl.BlockSpec(memory_space=pltpu.VMEM),
            pl.BlockSpec(memory_space=pl.ANY),
        ],
        out_specs=pl.BlockSpec(memory_space=pl.ANY),
        scratch_shapes=[
            vmem((cells, width), bf16),
            vmem((2 * bins, cells), bf16),
            vmem((2 * bins, width), bf16),
            vmem((full, full), bf16),
            vmem((full, full), bf16),
            vmem((full, full), bf16),
            vmem((full, full), f32),
            vmem((2 * full, full), f32),
            vmem((2 * full, full), bf16),
            vmem((full, half), f32),
            vmem((full, half), f32),
            vmem((full, half), f32),
            vmem((bins, full), f32),
            vmem((bins, full), f32),
            dma((cells // block,)),
            dma((cells // block,)),
        ],
        name="solve",
    )(parts, doppler, snaps)


def per_device(snapshots, training, doppler):
    snaps = snapshots[0]
    block = min(4096, snaps.shape[0])
    packed = gram(snaps, training[None, :], block)
    parts = all_sum(packed)
    return solve(parts, doppler[0][:, None], snaps, lax.axis_size("bins"), 1024)[None]


def solution(mesh):
    in_specs = (P("bins", "cells", None), P("cells"), P("bins", None))
    out_specs = P("bins", None, "cells")
    return jax.shard_map(
        per_device, mesh=mesh, in_specs=in_specs, out_specs=out_specs, check_vma=False
    )
```

```python
import functools
import math

import jax
import jax.numpy as jnp
from jax import lax
from jax.experimental import pallas as pl
from jax.experimental.pallas import tpu as pltpu
from jax.sharding import PartitionSpec as P

CHANNELS = 16
PULSES = 16
NDOPP = 1024


load_ratio = 0.5
look_freq = 0.125

EXTRA = 8
HIGH = lax.Precision.HIGH
MESH = pl.DeviceIdType.MESH


def sum_kernel(
    n, m, chunks, blocks, keep_hbm, x_hbm, out_ref,
    keep_ref, x_buf, acc, cross, packed, rs_buf, tr_src, tr_buf, mine, keep_sem, in_sems, sems,
):
    me = lax.axis_index("cells")
    g = lax.axis_index("bins")
    cells, width = x_buf.shape
    half = width // 2
    side = half // 2
    rows = half // (n * chunks)
    rs_send, rs_recv, tr_send, tr_recv, ag_send, ag_recv = sems
    block = cells // blocks

    for k in range(blocks):
        span = pl.ds(k * block, block)
        copy = pltpu.make_async_copy(x_hbm.at[span], x_buf.at[span], in_sems.at[k])
        copy.start()

    keep_copy = pltpu.make_async_copy(keep_hbm, keep_ref, keep_sem)
    keep_copy.start()
    barrier = pltpu.get_barrier_semaphore()
    for k in range(1, n):
        pl.semaphore_signal(
            barrier, inc=1, device_id=(lax.rem(me + k, n), g), device_id_type=MESH
        )
    for k in range(1, m):
        pl.semaphore_signal(
            barrier, inc=1, device_id=(me, lax.rem(g + k, m)), device_id_type=MESH
        )

    r = lax.broadcasted_iota(jnp.int32, (side, side), 0)
    c = lax.broadcasted_iota(jnp.int32, (side, side), 1)

    def products(part, k):
        span = pl.ds(pl.multiple_of(k * block, block), block)
        keep = keep_ref[:, span].astype(jnp.bfloat16)
        mr = x_buf[span, part * side:(part + 1) * side].T * keep
        mi = x_buf[span, half + part * side:half + (part + 1) * side].T * keep
        both = jnp.dot(
            jnp.concatenate([mr, mi], 0), x_buf[span, half:], preferred_element_type=jnp.float32
        )
        real = jnp.dot(mr, x_buf[span, :half], preferred_element_type=jnp.float32)
        acc[:half, :] += both
        acc[half:, :] += real

    def send(k):
        for j in range(1, n):
            peer = lax.rem(me + j, n)
            copy = pltpu.make_async_remote_copy(
                src_ref=packed.at[pl.ds(pl.multiple_of((k * n + peer) * rows, rows), rows)],
                dst_ref=rs_buf.at[k, j - 1],
                send_sem=rs_send.at[k, j - 1],
                recv_sem=rs_recv.at[k, j - 1],
                device_id=(peer, g),
                device_id_type=MESH,
            )
            copy.start()
            scatters.append(copy)

    scatters = []
    keep_copy.wait()

    def fresh(k, _):
        span = pl.ds(pl.multiple_of(k * block, block), block)
        pltpu.make_async_copy(x_hbm.at[span], x_buf.at[span], in_sems.at[k]).wait()
        products(0, k)
        return 0

    acc[...] = jnp.zeros_like(acc)
    lax.fori_loop(0, blocks, fresh, 0)
    cr = acc[:side, :]
    re = acc[side:half, :] + acc[half:, :]
    cross[...] = cr[:, side:]
    packed[:side, :side] = jnp.where(r <= c, re[:, :side], cr[:, :side].T - cr[:, :side])
    packed[:side, side:] = re[:, side:]
    trace = jnp.sum(jnp.where(r == c, re[:, :side], 0.0), axis=0, keepdims=True)
    pl.semaphore_wait(barrier, n + m - 2)
    early = chunks // 2
    for k in range(early):
        send(k)

    def again(k, _):
        products(1, k)
        return 0

    acc[...] = jnp.zeros_like(acc)
    lax.fori_loop(0, blocks, again, 0)
    cr = acc[:side, :]
    re = acc[side:half, side:] + acc[half:, side:]
    packed[side:, :side] = cross[...].T - cr[:, :side]
    packed[side:, side:] = jnp.where(r <= c, re, cr[:, side:].T - cr[:, side:])
    trace = trace + jnp.sum(jnp.where(r == c, re, 0.0), axis=0, keepdims=True)
    tr_src[...] = jnp.broadcast_to(trace, tr_src.shape)
    traces = []
    for k in range(1, m):
        copy = pltpu.make_async_remote_copy(
            src_ref=tr_src,
            dst_ref=tr_buf.at[k - 1],
            send_sem=tr_send.at[k - 1],
            recv_sem=tr_recv.at[k - 1],
            device_id=(me, lax.rem(g + k, m)),
            device_id_type=MESH,
        )
        copy.start()
        traces.append(copy)
    for k in range(early, chunks):
        send(k)

    gathers = []
    for k in range(chunks):
        for copy in scatters[k * (n - 1):(k + 1) * (n - 1)]:
            copy.wait()
        total = packed[pl.ds(pl.multiple_of((k * n + me) * rows, rows), rows), :]
        for j in range(n - 1):
            total = total + rs_buf[k, j]
        mine[k, :rows, :] = total
        out_ref[k, me, :rows, :] = total
        size = rows
        if k == chunks - 1:
            for copy in traces:
                copy.wait()
            power = tr_src[...]
            for j in range(m - 1):
                power = power + tr_buf[j]
            mine[k, rows:, :side] = power
            out_ref[k, me, rows:, :side] = power
            mine[k, rows:, side:] = jnp.zeros_like(power)
            size = rows + EXTRA
        for j in range(1, n):
            copy = pltpu.make_async_remote_copy(
                src_ref=mine.at[k, pl.ds(0, size)],
                dst_ref=out_ref.at[k, me, pl.ds(0, size)],
                send_sem=ag_send.at[k, j - 1],
                recv_sem=ag_recv.at[k, j - 1],
                device_id=(lax.rem(me + j, n), g),
                device_id_type=MESH,
            )
            copy.start()
            gathers.append((k, j, size, copy))
    for k, j, size, copy in gathers:
        copy.wait_send()
        peer = lax.rem(me + n - j, n)
        pltpu.make_async_remote_copy(
            src_ref=mine.at[k, pl.ds(0, size)],
            dst_ref=out_ref.at[k, peer, pl.ds(0, size)],
            send_sem=ag_send.at[k, j - 1],
            recv_sem=ag_recv.at[k, j - 1],
            device_id=(peer, g),
            device_id_type=MESH,
        ).wait_recv()


def gram_sum(snaps, keep):
    n, m = lax.axis_size("cells"), lax.axis_size("bins")
    cells, width = snaps.shape
    half = width // 2
    side = half // 2
    chunks = max(1, min(CHUNKS, half // (8 * n)))
    rows = half // (n * chunks)
    blocks = max(1, cells // 1024)
    dma = pltpu.SemaphoreType.DMA
    f32, vmem = jnp.float32, pltpu.VMEM
    return pl.pallas_call(
        functools.partial(sum_kernel, n, m, chunks, blocks),
        out_shape=jax.ShapeDtypeStruct((chunks, n, rows + EXTRA, half), f32),
        in_specs=[pl.BlockSpec(memory_space=pltpu.HBM)] * 2,
        out_specs=pl.BlockSpec(memory_space=pltpu.VMEM),
        scratch_shapes=[
            vmem((1, cells), jnp.int32),
            vmem((cells, width), jnp.bfloat16),
            vmem((half + side, half), f32),
            vmem((side, side), f32),
            vmem((half, half), f32),
            vmem((chunks, n - 1, rows, half), f32),
            vmem((EXTRA, side), f32),
            vmem((m - 1, EXTRA, side), f32),
            vmem((chunks, rows + EXTRA, half), f32),
            dma(()),
            dma((blocks,)),
            [dma((chunks, n - 1)), dma((chunks, n - 1)), dma((m - 1,)), dma((m - 1,)), dma((chunks, n - 1)), dma((chunks, n - 1))],
        ],
        compiler_params=pltpu.CompilerParams(
            collective_id=0, has_side_effects=True, vmem_limit_bytes=VMEM_LIMIT
        ),
        name="gram_sum",
    )(keep, snaps)


def grow(d):
    return (4.0 * d - 2.0 * d * d) / (1.0 + 2.0 * d - d * d)


def start_for(steps, goal):
    lo, hi = 0.0, 1.0
    for _ in range(100):
        mid = 0.5 * (lo + hi)
        d = mid
        for _ in range(steps):
            d = grow(d)
        lo, hi = (lo, mid) if d >= goal else (mid, hi)
    return hi


def split(x, parts):
    out = []
    for _ in range(parts):
        top = x.astype(jnp.bfloat16)
        out.append(top)
        x = x - top.astype(jnp.float32)
    return out


def mxu(a, b):
    return jnp.dot(a, b, preferred_element_type=jnp.float32)


def total(x):
    return jnp.sum(jnp.sum(x, axis=0, keepdims=True), axis=1, keepdims=True)


def steer_rows(doppler, chans, pulses):
    bins, dim = doppler.shape[1], chans * pulses
    at = lax.broadcasted_iota(jnp.int32, (bins, bins), 0)
    to = lax.broadcasted_iota(jnp.int32, (bins, bins), 1)
    doppler = jnp.sum(
        jnp.where(at == to, doppler.astype(jnp.float32), 0.0), axis=1, keepdims=True
    )
    index = lax.broadcasted_iota(jnp.int32, (1, dim), 1)
    pulse = lax.rem(index, pulses)
    chan = ((index - pulse) // pulses).astype(jnp.float32)
    freq = doppler * (1.0 / NDOPP) - 0.5
    turns = look_freq * chan + pulse.astype(jnp.float32) * freq
    phase = (2.0 * math.pi) * turns
    quarter = jnp.floor(4.0 * turns + 0.5)
    rest = phase - quarter * 1.5703125
    rest = rest - quarter * 4.837512969970703125e-4
    rest = rest - quarter * 7.549789948768648e-8
    sq = rest * rest
    sin = rest + rest * sq * (
        -1.6666654611e-1 + sq * (8.3321608736e-3 + sq * -1.9515295891e-4)
    )
    cos = 1.0 + sq * (
        -0.5 + sq * (4.166664568298827e-2 + sq * (-1.388731625493765e-3 + sq * 2.443315711809948e-5))
    )
    which = quarter.astype(jnp.int32) & 3
    odd = (which & 1) == 1
    c = jnp.where(odd, sin, cos)
    s = jnp.where(odd, cos, sin)
    c = jnp.where((which == 1) | (which == 2), -c, c)
    s = jnp.where(which >= 2, -s, s)
    return jnp.concatenate([c, s], 1) * (1.0 / math.sqrt(dim))


def solve_kernel(
    groups, block, parts_ref, dop_hbm, x_hbm, out_hbm,
    dop, x_buf, out_buf, taps, re_parts, im_parts, pair, wide, xs, ys, acol, steer, w_ref,
    dop_sem, in_sems, out_sems,
):
    chunks, n = parts_ref.shape[:2]
    rows = parts_ref.shape[2] - EXTRA
    half = parts_ref.shape[3]
    full = 2 * half
    bins = dop.shape[1]
    cells = x_buf.shape[0]
    f32, bf16 = jnp.float32, jnp.bfloat16

    dop_copy = pltpu.make_async_copy(dop_hbm, dop, dop_sem)
    dop_copy.start()
    loads = []
    for k in range(cells // block):
        span = pl.ds(k * block, block)
        copy = pltpu.make_async_copy(x_hbm.at[span], x_buf.at[span], in_sems.at[k])
        copy.start()
        loads.append(copy)

    summed = jnp.concatenate(
        [parts_ref[k, j, :rows, :] for k in range(chunks) for j in range(n)], 0
    )
    power_row = parts_ref[chunks - 1, 0, rows:rows + 1, :half // 2]
    for k in range(1, n):
        power_row = power_row + parts_ref[chunks - 1, k, rows:rows + 1, :half // 2]
    noise = jnp.sum(power_row, axis=1, keepdims=True) / (groups * half)
    low = load_ratio * noise
    r = lax.broadcasted_iota(jnp.int32, (half, half), 0)
    c = lax.broadcasted_iota(jnp.int32, (half, half), 1)
    trace = total(jnp.where(r == c, summed, 0.0))
    unit = 1.0 / (trace + low)
    norm = summed * unit
    norm = norm * norm
    fro = jnp.sqrt(total(jnp.where(r == c, norm, norm + norm))) * (trace + low)
    bound = jnp.minimum(trace, 1.0001 * fro)
    scale = 2.0 / (bound + 2.0 * low)
    eye = jnp.where(r == c, 1.0, 0.0)
    flip = summed.T
    real = (jnp.where(r <= c, summed, flip) + low * eye) * scale
    imag = jnp.where(r > c, summed, jnp.where(r < c, -flip, 0.0)) * scale
    acol[:half, :] = real
    acol[half:, :] = imag
    for k, (xr, xi) in enumerate(zip(split(real, 3), split(imag, 3))):
        re_parts[k * half:(k + 1) * half, :] = xr
        im_parts[k * half:(k + 1) * half, :] = xi
        if k == 0:
            pair[:half, :] = xr
            pair[half:full, :] = xi

    def times(left, re, im):
        rows = left.shape[0] // 2
        p, q = mxu(left, re), mxu(left, im)
        return p[:rows] - q[rows:], p[rows:] + q[:rows]

    square = jnp.concatenate(times(pair[:full, :], re_parts[:half, :], im_parts[:half, :]), 0)
    top = total(square * square)
    dop_copy.wait()
    steer[...] = steer_rows(dop[...], CHANNELS, PULSES)

    lam = 1.005 * jnp.sqrt(jnp.sqrt(top)) / scale - low
    tight = jnp.minimum(bound, jnp.maximum(lam, 0.0))
    gainup = (bound + 2.0 * low) / (tight + 2.0 * low)
    d0 = 2.0 * low / (tight + 2.0 * low)

    def bend_of(d):
        return 2.0 / (1.0 + 2.0 * d - d * d)

    def pack(at, v):
        pair[at * half:at * half + full, :] = v.astype(bf16)

    def first(square, d):
        bend = bend_of(d)
        a = acol[...] * (bend * gainup)
        x1 = -a
        xs[...] = jnp.concatenate([x1[:half] + (2.0 * bend) * eye, x1[half:]], 0)
        ys[...] = 2.0 * a - square * (bend * gainup * gainup)
        return grow(d)

    def steps_of(d):
        count = jnp.zeros_like(d)
        for k in range(2, 12):
            count = count + jnp.where(d < START[k], 1.0, 0.0)
        return jnp.max(count).astype(jnp.int32)

    coarse = jnp.max(jnp.where(d0 < COARSE, 1.0, 0.0)) > 0.5

    @pl.when(jnp.logical_not(coarse))
    def _():
        d1 = first(square, d0)
        pack(0, xs[...])
        pack(2, ys[...])

        def body(_, d):
            bend = bend_of(d)
            p = mxu(pair[...], pair[full:full + half, :])
            q = mxu(pair[...], pair[full + half:, :])
            for at, ref in ((0, xs), (full, ys)):
                re = bend * (2.0 * ref[:half, :] - (p[at:at + half] - q[at + half:at + full]))
                im = bend * (2.0 * ref[half:, :] - (p[at + half:at + full] + q[at:at + half]))
                ref[:half, :] = re
                ref[half:, :] = im
                pair[at:at + half, :] = re.astype(bf16)
                pair[at + half:at + full, :] = im.astype(bf16)
            return grow(d)

        d = lax.fori_loop(0, steps_of(d0), body, d1)
        bend = bend_of(d)
        re, im = times(pair[:full, :], pair[full:full + half, :], pair[full + half:, :])
        pair[:half, :] = (bend * (2.0 * xs[:half, :] - re)).astype(bf16)
        pair[half:full, :] = (bend * (2.0 * xs[half:, :] - im)).astype(bf16)

    @pl.when(coarse)
    def _():
        def product(left, ref):
            wide[:half, :half] = left[:half]
            wide[half:, half:] = left[:half]
            wide[:half, half:] = -left[half:]
            wide[half:, :half] = left[half:]
            return jnp.dot(wide[...], ref[...], preferred_element_type=f32, precision=HIGH)

        d1 = first(product(acol[...], acol), d0)

        def body(_, d):
            bend = bend_of(d)
            xs[...] = bend * (2.0 * xs[...] - product(xs[...], ys))
            ys[...] = bend * (2.0 * ys[...] - product(ys[...], ys))
            return grow(d)

        lax.fori_loop(0, steps_of(d0) + 1, body, d1)
        pack(0, xs[...])

    def stack(v):
        return jnp.concatenate([v[:, :half], v[:, half:]], 0).astype(bf16)

    def apply(v):
        left = stack(v)
        p, q = mxu(left, pair[:half, :]), mxu(left, pair[half:full, :])
        return jnp.concatenate([p[:bins] + q[bins:], p[bins:] - q[:bins]], 1) * gainup

    def short(v):
        return v.astype(bf16).astype(f32)

    def less(rest, w, parts):
        left = jnp.concatenate([stack(w)] * parts, 1)
        p = mxu(left, re_parts[:parts * half, :])
        q = mxu(left, im_parts[:parts * half, :])
        return rest - jnp.concatenate([p[:bins] + q[bins:], p[bins:] - q[:bins]], 1)

    w0 = short(apply(steer[...]))
    rest = less(steer[...], w0, 3)
    w1 = short(apply(rest))
    rest = less(rest, w1, 3)
    w2 = short(apply(rest))
    rest = less(rest, w2, 2)
    w_ref[...] = w0 + (w1 + (w2 + apply(rest)))

    @pl.when(coarse)
    def _():
        def body(_, w):
            rest = steer[...]
            for part in split(w, 3):
                rest = less(rest, part.astype(f32), 3)
            return w + apply(rest)
        w_ref[...] = lax.fori_loop(0, 4, body, w_ref[...])

    w = w_ref[...]
    gain = jnp.sum(steer[...] * w, axis=1, keepdims=True)
    w = w / gain
    wr, wi = w[:, :half], w[:, half:]
    taps[:bins, :half] = wr.astype(bf16)
    taps[:bins, half:] = wi.astype(bf16)
    taps[bins:, :half] = (-wi).astype(bf16)
    taps[bins:, half:] = wr.astype(bf16)

    for copy in loads:
        copy.wait()
    stores = []
    for k in range(cells // block):
        span = pl.ds(k * block, block)
        out_buf[:, span] = lax.dot_general(
            taps[...], x_buf[span, :], (((1,), (1,)), ((), ())), preferred_element_type=f32
        ).astype(bf16)
        copy = pltpu.make_async_copy(out_buf.at[:, span], out_hbm.at[:, span], out_sems.at[k])
        copy.start()
        stores.append(copy)
    for copy in stores:
        copy.wait()


GOAL = 0.95
START = [start_for(k, GOAL) for k in range(12)]
COARSE = 0.005
CHUNKS = 2
VMEM_LIMIT = 52 * 1024 * 1024


def solve(parts, doppler, snaps, groups, block):
    half = parts.shape[3]
    bins = doppler.shape[1]
    cells, width = snaps.shape
    full = 2 * half
    f32, bf16 = jnp.float32, jnp.bfloat16
    vmem = pltpu.VMEM
    dma = pltpu.SemaphoreType.DMA
    return pl.pallas_call(
        functools.partial(solve_kernel, groups, block),
        out_shape=jax.ShapeDtypeStruct((2 * bins, cells), bf16),
        in_specs=[
            pl.BlockSpec(memory_space=pltpu.VMEM),
            pl.BlockSpec(memory_space=pltpu.HBM),
            pl.BlockSpec(memory_space=pltpu.HBM),
        ],
        out_specs=pl.BlockSpec(memory_space=pltpu.HBM),
        scratch_shapes=[
            vmem((1, bins), jnp.int32),
            vmem((cells, width), bf16),
            vmem((2 * bins, cells), bf16),
            vmem((2 * bins, width), bf16),
            vmem((3 * half, half), bf16),
            vmem((3 * half, half), bf16),
            vmem((2 * full, half), bf16),
            vmem((full, full), f32),
            vmem((full, half), f32),
            vmem((full, half), f32),
            vmem((full, half), f32),
            vmem((bins, full), f32),
            vmem((bins, full), f32),
            dma(()),
            dma((cells // block,)),
            dma((cells // block,)),
        ],
        compiler_params=pltpu.CompilerParams(vmem_limit_bytes=VMEM_LIMIT),
        name="solve",
    )(parts, doppler, snaps)


def per_device(snapshots, training, doppler):
    snaps = snapshots[0]
    parts = gram_sum(snaps, training[None, :])
    return solve(parts, doppler, snaps, lax.axis_size("bins"), 1024)[None]


def solution(mesh):
    in_specs = (P("bins", "cells", None), P("cells"), P("bins", None))
    out_specs = P("bins", None, "cells")
    return jax.shard_map(
        per_device, mesh=mesh, in_specs=in_specs, out_specs=out_specs, check_vma=False
    )
```

```python
import functools
import math

import jax
import jax.numpy as jnp
from jax import lax
from jax.experimental import pallas as pl
from jax.experimental.pallas import tpu as pltpu
from jax.sharding import PartitionSpec as P

CHANNELS = 16
PULSES = 16
NDOPP = 1024


load_ratio = 0.5
look_freq = 0.125

HIGH = lax.Precision.HIGH
MESH = pl.DeviceIdType.MESH


def sum_kernel(
    n, m, chunks, blocks, keep_hbm, x_hbm, out_ref, pw_ref,
    keep_ref, x_buf, acc, late, cross, packed, rs_buf, tr_src, tr_buf, pw_src, mine, keep_sem, in_sems, sems,
):
    me = lax.axis_index("cells")
    g = lax.axis_index("bins")
    cells, width = x_buf.shape
    half = width // 2
    side = half // 2
    rows = half // (n * chunks)
    rs_send, rs_recv, tr_send, tr_recv, pw_send, pw_recv, ag_send, ag_recv = sems
    block = cells // blocks

    for k in range(min(DEPTH, blocks)):
        span = pl.ds(k * block, block)
        pltpu.make_async_copy(x_hbm.at[span], x_buf.at[span], in_sems.at[k]).start()
    keep_copy = pltpu.make_async_copy(keep_hbm, keep_ref, keep_sem)
    keep_copy.start()
    barrier = pltpu.get_barrier_semaphore()
    for k in range(1, n):
        pl.semaphore_signal(
            barrier, inc=1, device_id=(lax.rem(me + k, n), g), device_id_type=MESH
        )
    for k in range(1, m):
        pl.semaphore_signal(
            barrier, inc=1, device_id=(me, lax.rem(g + k, m)), device_id_type=MESH
        )

    r = lax.broadcasted_iota(jnp.int32, (side, side), 0)
    c = lax.broadcasted_iota(jnp.int32, (side, side), 1)

    def turned(span, at):
        return x_buf[span, at:at + side].T * keep_ref[:, span].astype(jnp.bfloat16)

    def load(k):
        span = pl.ds(pl.multiple_of(k * block, block), block)
        return pltpu.make_async_copy(x_hbm.at[span], x_buf.at[span], in_sems.at[k])

    def send(k):
        for j in range(1, n):
            peer = lax.rem(me + j, n)
            copy = pltpu.make_async_remote_copy(
                src_ref=packed.at[pl.ds(pl.multiple_of((k * n + peer) * rows, rows), rows)],
                dst_ref=rs_buf.at[k, j - 1],
                send_sem=rs_send.at[k, j - 1],
                recv_sem=rs_recv.at[k, j - 1],
                device_id=(peer, g),
                device_id_type=MESH,
            )
            copy.start()
            scatters.append(copy)

    scatters = []
    keep_copy.wait()

    def fresh(k, _):
        load(k).wait()

        @pl.when(k + DEPTH < blocks)
        def _():
            load(k + DEPTH).start()

        span = pl.ds(pl.multiple_of(k * block, block), block)
        mr = turned(span, 0)
        left = jnp.concatenate([mr, turned(span, half), turned(span, half + side)], 0)
        acc[:3 * side, :] += jnp.dot(left, x_buf[span, half:], preferred_element_type=jnp.float32)
        acc[3 * side:, :] += jnp.dot(mr, x_buf[span, :half], preferred_element_type=jnp.float32)
        return 0

    acc[...] = jnp.zeros_like(acc)
    late[...] = jnp.zeros_like(late)
    lax.fori_loop(0, blocks, fresh, 0)
    cr = acc[:side, :]
    re = acc[side:half, :] + acc[3 * side:, :]
    cross[...] = cr[:, side:]
    packed[:side, :side] = jnp.where(r <= c, re[:, :side], cr[:, :side].T - cr[:, :side])
    packed[:side, side:] = re[:, side:]
    trace = jnp.sum(jnp.where(r == c, re[:, :side], 0.0), axis=0, keepdims=True)
    pl.semaphore_wait(barrier, n + m - 2)
    early = chunks // 2
    for k in range(early):
        send(k)

    def again(k, _):
        span = pl.ds(pl.multiple_of(k * wide, wide), wide)
        late[...] += jnp.dot(turned(span, side), x_buf[span, :], preferred_element_type=jnp.float32)
        return 0

    wide = min(WIDE, cells)
    lax.fori_loop(0, cells // wide, again, 0)
    cr = late[:, half:]
    re = acc[half:half + side, side:] + late[:, side:half]
    packed[side:, :side] = cross[...].T - cr[:, :side]
    packed[side:, side:] = jnp.where(r <= c, re, cr[:, side:].T - cr[:, side:])
    trace = trace + jnp.sum(jnp.where(r == c, re, 0.0), axis=0, keepdims=True)
    tr_src[...] = trace
    traces = []
    for k in range(1, m):
        copy = pltpu.make_async_remote_copy(
            src_ref=tr_src,
            dst_ref=tr_buf.at[k - 1],
            send_sem=tr_send.at[k - 1],
            recv_sem=tr_recv.at[k - 1],
            device_id=(me, lax.rem(g + k, m)),
            device_id_type=MESH,
        )
        copy.start()
        traces.append(copy)
    for k in range(early, chunks):
        send(k)

    gathers = []
    for k in range(chunks):
        if k == chunks - 1:
            for copy in traces:
                copy.wait()
            power = tr_src[...]
            for j in range(m - 1):
                power = power + tr_buf[j]
            both = jnp.concatenate([power, tr_src[...]], 0)
            pw_src[...] = both
            pw_ref[me] = both
            spread = []
            for j in range(1, n):
                copy = pltpu.make_async_remote_copy(
                    src_ref=pw_src,
                    dst_ref=pw_ref.at[me],
                    send_sem=pw_send.at[j - 1],
                    recv_sem=pw_recv.at[j - 1],
                    device_id=(lax.rem(me + j, n), g),
                    device_id_type=MESH,
                )
                copy.start()
                spread.append(copy)
        for copy in scatters[k * (n - 1):(k + 1) * (n - 1)]:
            copy.wait()
        total = packed[pl.ds(pl.multiple_of((k * n + me) * rows, rows), rows), :]
        for j in range(n - 1):
            total = total + rs_buf[k, j]
        mine[k] = total
        out_ref[k, me] = total
        for j in range(1, n):
            copy = pltpu.make_async_remote_copy(
                src_ref=mine.at[k],
                dst_ref=out_ref.at[k, me],
                send_sem=ag_send.at[k, j - 1],
                recv_sem=ag_recv.at[k, j - 1],
                device_id=(lax.rem(me + j, n), g),
                device_id_type=MESH,
            )
            copy.start()
            gathers.append((k, j, copy))
    for j in range(1, n):
        spread[j - 1].wait_send()
        peer = lax.rem(me + n - j, n)
        pltpu.make_async_remote_copy(
            src_ref=pw_src,
            dst_ref=pw_ref.at[peer],
            send_sem=pw_send.at[j - 1],
            recv_sem=pw_recv.at[j - 1],
            device_id=(peer, g),
            device_id_type=MESH,
        ).wait_recv()
    for k, j, copy in gathers:
        copy.wait_send()
        peer = lax.rem(me + n - j, n)
        pltpu.make_async_remote_copy(
            src_ref=mine.at[k],
            dst_ref=out_ref.at[k, peer],
            send_sem=ag_send.at[k, j - 1],
            recv_sem=ag_recv.at[k, j - 1],
            device_id=(peer, g),
            device_id_type=MESH,
        ).wait_recv()


def gram_sum(snaps, keep):
    n, m = lax.axis_size("cells"), lax.axis_size("bins")
    cells, width = snaps.shape
    half = width // 2
    side = half // 2
    chunks = max(1, min(CHUNKS, half // (8 * n)))
    rows = half // (n * chunks)
    blocks = max(1, cells // BLOCK)
    dma = pltpu.SemaphoreType.DMA
    f32, vmem = jnp.float32, pltpu.VMEM
    return pl.pallas_call(
        functools.partial(sum_kernel, n, m, chunks, blocks),
        out_shape=(
            jax.ShapeDtypeStruct((chunks, n, rows, half), f32),
            jax.ShapeDtypeStruct((n, 2, side), f32),
        ),
        in_specs=[pl.BlockSpec(memory_space=pltpu.HBM)] * 2,
        out_specs=(pl.BlockSpec(memory_space=pltpu.VMEM),) * 2,
        scratch_shapes=[
            vmem((1, cells), jnp.int32),
            vmem((cells, width), jnp.bfloat16),
            vmem((4 * side, half), f32),
            vmem((side, width), f32),
            vmem((side, side), f32),
            vmem((half, half), f32),
            vmem((chunks, n - 1, rows, half), f32),
            vmem((1, side), f32),
            vmem((m - 1, 1, side), f32),
            vmem((2, side), f32),
            vmem((chunks, rows, half), f32),
            dma(()),
            dma((blocks,)),
            [dma((chunks, n - 1)), dma((chunks, n - 1)), dma((m - 1,)), dma((m - 1,)), dma((n - 1,)), dma((n - 1,)), dma((chunks, n - 1)), dma((chunks, n - 1))],
        ],
        compiler_params=pltpu.CompilerParams(
            collective_id=0, has_side_effects=True, vmem_limit_bytes=VMEM_LIMIT
        ),
        name="gram_sum",
    )(keep, snaps)


def grow(d):
    return (4.0 * d - 2.0 * d * d) / (1.0 + 2.0 * d - d * d)


def start_for(steps, goal):
    lo, hi = 0.0, 1.0
    for _ in range(100):
        mid = 0.5 * (lo + hi)
        d = mid
        for _ in range(steps):
            d = grow(d)
        lo, hi = (lo, mid) if d >= goal else (mid, hi)
    return hi


def split(x, parts):
    out = []
    for _ in range(parts):
        top = x.astype(jnp.bfloat16)
        out.append(top)
        x = x - top.astype(jnp.float32)
    return out


def mxu(a, b):
    return jnp.dot(a, b, preferred_element_type=jnp.float32)


def total(x):
    return jnp.sum(jnp.sum(x, axis=0, keepdims=True), axis=1, keepdims=True)


def steer_rows(doppler, chans, pulses):
    bins, dim = doppler.shape[1], chans * pulses
    at = lax.broadcasted_iota(jnp.int32, (bins, bins), 0)
    to = lax.broadcasted_iota(jnp.int32, (bins, bins), 1)
    doppler = jnp.sum(
        jnp.where(at == to, doppler.astype(jnp.float32), 0.0), axis=1, keepdims=True
    )
    index = lax.broadcasted_iota(jnp.int32, (1, dim), 1)
    pulse = lax.rem(index, pulses)
    chan = ((index - pulse) // pulses).astype(jnp.float32)
    freq = doppler * (1.0 / NDOPP) - 0.5
    turns = look_freq * chan + pulse.astype(jnp.float32) * freq
    phase = (2.0 * math.pi) * turns
    quarter = jnp.floor(4.0 * turns + 0.5)
    rest = phase - quarter * 1.5703125
    rest = rest - quarter * 4.837512969970703125e-4
    rest = rest - quarter * 7.549789948768648e-8
    sq = rest * rest
    sin = rest + rest * sq * (
        -1.6666654611e-1 + sq * (8.3321608736e-3 + sq * -1.9515295891e-4)
    )
    cos = 1.0 + sq * (
        -0.5 + sq * (4.166664568298827e-2 + sq * (-1.388731625493765e-3 + sq * 2.443315711809948e-5))
    )
    which = quarter.astype(jnp.int32) & 3
    odd = (which & 1) == 1
    c = jnp.where(odd, sin, cos)
    s = jnp.where(odd, cos, sin)
    c = jnp.where((which == 1) | (which == 2), -c, c)
    s = jnp.where(which >= 2, -s, s)
    return jnp.concatenate([c, s], 1) * (1.0 / math.sqrt(dim))


def solve_kernel(
    groups, block, sum_ref, pw_ref, dop_hbm, x_hbm, out_hbm,
    dop, x_buf, out_buf, taps, re_parts, im_parts, pair, wide, xs, ys, acol, steer, w_ref,
    dop_sem, in_sems, out_sems,
):
    half = sum_ref.shape[0]
    full = 2 * half
    bins = dop.shape[1]
    cells = x_buf.shape[0]
    f32, bf16 = jnp.float32, jnp.bfloat16

    dop_copy = pltpu.make_async_copy(dop_hbm, dop, dop_sem)
    dop_copy.start()
    loads = []
    for k in range(cells // block):
        span = pl.ds(k * block, block)
        copy = pltpu.make_async_copy(x_hbm.at[span], x_buf.at[span], in_sems.at[k])
        copy.start()
        loads.append(copy)

    power = pw_ref[0]
    for k in range(1, pw_ref.shape[0]):
        power = power + pw_ref[k]
    power = jnp.sum(power, axis=1, keepdims=True)
    low = (load_ratio / (groups * half)) * power[:1]
    bound = 1.0001 * power[1:]
    scale = 2.0 / (bound + 2.0 * low)
    side = half // 2
    r = lax.broadcasted_iota(jnp.int32, (side, side), 0)
    c = lax.broadcasted_iota(jnp.int32, (side, side), 1)
    eye = jnp.where(r == c, 1.0, 0.0)

    def put(i, j, xr, xi):
        at, to = slice(i * side, (i + 1) * side), slice(j * side, (j + 1) * side)
        acol[at, to] = xr
        acol[half + i * side:half + (i + 1) * side, to] = xi
        for k, (tr, ti) in enumerate(zip(split(xr, 3), split(xi, 3))):
            re_parts[k * half + i * side:k * half + (i + 1) * side, to] = tr
            im_parts[k * half + i * side:k * half + (i + 1) * side, to] = ti
            if k == 0:
                pair[at, to] = tr
                pair[half + i * side:half + (i + 1) * side, to] = ti

    for i in range(2):
        own = sum_ref[i * side:(i + 1) * side, i * side:(i + 1) * side]
        flip = own.T
        xr = (jnp.where(r <= c, own, flip) + low * eye) * scale
        xi = jnp.where(r > c, own, jnp.where(r < c, -flip, 0.0)) * scale
        put(i, i, xr, xi)
    upper = sum_ref[:side, side:] * scale
    lower = sum_ref[side:, :side] * scale
    put(0, 1, upper, -lower.T)
    put(1, 0, upper.T, lower)

    def times(left, re, im):
        rows = left.shape[0] // 2
        p, q = mxu(left, re), mxu(left, im)
        return p[:rows] - q[rows:], p[rows:] + q[:rows]

    square = jnp.concatenate(times(pair[:full, :], re_parts[:half, :], im_parts[:half, :]), 0)
    top = total(square * square)
    dop_copy.wait()
    steer[...] = steer_rows(dop[...], CHANNELS, PULSES)

    lam = 1.005 * jnp.sqrt(jnp.sqrt(top)) / scale - low
    tight = jnp.minimum(bound, jnp.maximum(lam, 0.0))
    gainup = (bound + 2.0 * low) / (tight + 2.0 * low)
    d0 = 2.0 * low / (tight + 2.0 * low)

    def bend_of(d):
        return 2.0 / (1.0 + 2.0 * d - d * d)

    def pack(at, v):
        pair[at * half:at * half + full, :] = v.astype(bf16)

    def first(square, d):
        bend = bend_of(d)
        a = acol[...] * (bend * gainup)
        x1 = -a
        xs[...] = x1
        for i in range(2):
            at = slice(i * side, (i + 1) * side)
            xs[at, at] = x1[at, at] + (2.0 * bend) * eye
        ys[...] = 2.0 * a - square * (bend * gainup * gainup)
        return grow(d)

    def steps_of(d):
        count = jnp.zeros_like(d)
        for k in range(2, 12):
            count = count + jnp.where(d < START[k], 1.0, 0.0)
        return jnp.max(count).astype(jnp.int32)

    coarse = jnp.max(jnp.where(d0 < COARSE, 1.0, 0.0)) > 0.5

    @pl.when(jnp.logical_not(coarse))
    def _():
        d1 = first(square, d0)
        pack(0, xs[...])
        pack(2, ys[...])

        def body(_, d):
            bend = bend_of(d)
            p = mxu(pair[...], pair[full:full + half, :])
            q = mxu(pair[...], pair[full + half:, :])
            for at, ref in ((0, xs), (full, ys)):
                re = bend * (2.0 * ref[:half, :] - (p[at:at + half] - q[at + half:at + full]))
                im = bend * (2.0 * ref[half:, :] - (p[at + half:at + full] + q[at:at + half]))
                ref[:half, :] = re
                ref[half:, :] = im
                pair[at:at + half, :] = re.astype(bf16)
                pair[at + half:at + full, :] = im.astype(bf16)
            return grow(d)

        d = lax.fori_loop(0, steps_of(d0), body, d1)
        bend = bend_of(d)
        re, im = times(pair[:full, :], pair[full:full + half, :], pair[full + half:, :])
        pair[:half, :] = (bend * (2.0 * xs[:half, :] - re)).astype(bf16)
        pair[half:full, :] = (bend * (2.0 * xs[half:, :] - im)).astype(bf16)

    @pl.when(coarse)
    def _():
        def product(left, ref):
            wide[:half, :half] = left[:half]
            wide[half:, half:] = left[:half]
            wide[:half, half:] = -left[half:]
            wide[half:, :half] = left[half:]
            return jnp.dot(wide[...], ref[...], preferred_element_type=f32, precision=HIGH)

        d1 = first(product(acol[...], acol), d0)

        def body(_, d):
            bend = bend_of(d)
            xs[...] = bend * (2.0 * xs[...] - product(xs[...], ys))
            ys[...] = bend * (2.0 * ys[...] - product(ys[...], ys))
            return grow(d)

        lax.fori_loop(0, steps_of(d0) + 1, body, d1)
        pack(0, xs[...])

    def stack(v):
        return jnp.concatenate([v[:, :half], v[:, half:]], 0).astype(bf16)

    def apply(v):
        left = stack(v)
        p, q = mxu(left, pair[:half, :]), mxu(left, pair[half:full, :])
        return jnp.concatenate([p[:bins] + q[bins:], p[bins:] - q[:bins]], 1) * gainup

    def short(v):
        return v.astype(bf16).astype(f32)

    def less(rest, w, parts):
        left = jnp.concatenate([stack(w)] * parts, 1)
        p = mxu(left, re_parts[:parts * half, :])
        q = mxu(left, im_parts[:parts * half, :])
        return rest - jnp.concatenate([p[:bins] + q[bins:], p[bins:] - q[:bins]], 1)

    w0 = short(apply(steer[...]))
    rest = less(steer[...], w0, 3)
    w1 = short(apply(rest))
    rest = less(rest, w1, 3)
    w2 = short(apply(rest))
    rest = less(rest, w2, 2)
    w_ref[...] = w0 + (w1 + (w2 + apply(rest)))

    @pl.when(coarse)
    def _():
        def body(_, w):
            rest = steer[...]
            for part in split(w, 3):
                rest = less(rest, part.astype(f32), 3)
            return w + apply(rest)
        w_ref[...] = lax.fori_loop(0, 4, body, w_ref[...])

    w = w_ref[...]
    gain = jnp.sum(steer[...] * w, axis=1, keepdims=True)
    w = w / gain
    wr, wi = w[:, :half], w[:, half:]
    taps[:bins, :half] = wr.astype(bf16)
    taps[:bins, half:] = wi.astype(bf16)
    taps[bins:, :half] = (-wi).astype(bf16)
    taps[bins:, half:] = wr.astype(bf16)

    for copy in loads:
        copy.wait()
    stores = []
    for k in range(cells // block):
        span = pl.ds(k * block, block)
        out_buf[:, span] = lax.dot_general(
            taps[...], x_buf[span, :], (((1,), (1,)), ((), ())), preferred_element_type=f32
        ).astype(bf16)
        copy = pltpu.make_async_copy(out_buf.at[:, span], out_hbm.at[:, span], out_sems.at[k])
        copy.start()
        stores.append(copy)
    for copy in stores:
        copy.wait()


GOAL = 0.95
START = [start_for(k, GOAL) for k in range(12)]
COARSE = 0.005
CHUNKS = 2
DEPTH = 8
BLOCK = 2048
WIDE = 4096
VMEM_LIMIT = 52 * 1024 * 1024


def solve(summed, power, doppler, snaps, groups, block):
    half = summed.shape[0]
    bins = doppler.shape[1]
    cells, width = snaps.shape
    full = 2 * half
    f32, bf16 = jnp.float32, jnp.bfloat16
    vmem = pltpu.VMEM
    dma = pltpu.SemaphoreType.DMA
    return pl.pallas_call(
        functools.partial(solve_kernel, groups, block),
        out_shape=jax.ShapeDtypeStruct((2 * bins, cells), bf16),
        in_specs=[
            pl.BlockSpec(memory_space=pltpu.VMEM),
            pl.BlockSpec(memory_space=pltpu.VMEM),
            pl.BlockSpec(memory_space=pltpu.HBM),
            pl.BlockSpec(memory_space=pltpu.HBM),
        ],
        out_specs=pl.BlockSpec(memory_space=pltpu.HBM),
        scratch_shapes=[
            vmem((1, bins), jnp.int32),
            vmem((cells, width), bf16),
            vmem((2 * bins, cells), bf16),
            vmem((2 * bins, width), bf16),
            vmem((3 * half, half), bf16),
            vmem((3 * half, half), bf16),
            vmem((2 * full, half), bf16),
            vmem((full, full), f32),
            vmem((full, half), f32),
            vmem((full, half), f32),
            vmem((full, half), f32),
            vmem((bins, full), f32),
            vmem((bins, full), f32),
            dma(()),
            dma((cells // block,)),
            dma((cells // block,)),
        ],
        compiler_params=pltpu.CompilerParams(vmem_limit_bytes=VMEM_LIMIT),
        name="solve",
    )(summed, power, doppler, snaps)


def per_device(snapshots, training, doppler):
    snaps = snapshots[0]
    keep = pltpu.with_memory_space_constraint(training[None, :], pltpu.HBM)
    parts, power = gram_sum(snaps, keep)
    half = parts.shape[3]
    summed = parts.reshape(half, half)
    return solve(summed, power, doppler, snaps, lax.axis_size("bins"), 1024)[None]


def solution(mesh):
    in_specs = (P("bins", "cells", None), P("cells"), P("bins", None))
    out_specs = P("bins", None, "cells")
    return jax.shard_map(
        per_device, mesh=mesh, in_specs=in_specs, out_specs=out_specs, check_vma=False
    )
```

```python
import functools
import math

import jax
import jax.numpy as jnp
from jax import lax
from jax.experimental import pallas as pl
from jax.experimental.pallas import tpu as pltpu
from jax.sharding import PartitionSpec as P

CHANNELS = 16
PULSES = 16
NDOPP = 1024


load_ratio = 0.5
look_freq = 0.125

HIGH = lax.Precision.HIGH
MESH = pl.DeviceIdType.MESH


def sum_kernel(
    n, m, chunks, blocks, keep_hbm, x_hbm, out_ref, pw_ref,
    keep_ref, x_buf, acc, late, cross, packed, rs_buf, tr_src, tr_buf, pw_src, mine, keep_sem, in_sems, sems,
):
    me = lax.axis_index("cells")
    g = lax.axis_index("bins")
    cells, width = x_buf.shape
    half = width // 2
    side = half // 2
    rows = half // (n * chunks)
    rs_send, rs_recv, tr_send, tr_recv, pw_send, pw_recv, ag_send, ag_recv = sems
    block = cells // blocks

    keep_copy = pltpu.make_async_copy(keep_hbm, keep_ref, keep_sem)
    keep_copy.start()
    for k in range(min(DEPTH, blocks)):
        span = pl.ds(k * block, block)
        pltpu.make_async_copy(x_hbm.at[span], x_buf.at[span], in_sems.at[k]).start()
    barrier = pltpu.get_barrier_semaphore()
    for k in range(1, n):
        pl.semaphore_signal(
            barrier, inc=1, device_id=(lax.rem(me + k, n), g), device_id_type=MESH
        )
    for k in range(1, m):
        pl.semaphore_signal(
            barrier, inc=1, device_id=(me, lax.rem(g + k, m)), device_id_type=MESH
        )

    r = lax.broadcasted_iota(jnp.int32, (side, side), 0)
    c = lax.broadcasted_iota(jnp.int32, (side, side), 1)

    def turned(span, at):
        return x_buf[span, at:at + side].T * keep_ref[:, span].astype(jnp.bfloat16)

    def load(k):
        span = pl.ds(pl.multiple_of(k * block, block), block)
        return pltpu.make_async_copy(x_hbm.at[span], x_buf.at[span], in_sems.at[k])

    def send(k):
        for j in range(1, n):
            peer = lax.rem(me + j, n)
            copy = pltpu.make_async_remote_copy(
                src_ref=packed.at[pl.ds(pl.multiple_of((k * n + peer) * rows, rows), rows)],
                dst_ref=rs_buf.at[k, j - 1],
                send_sem=rs_send.at[k, j - 1],
                recv_sem=rs_recv.at[k, j - 1],
                device_id=(peer, g),
                device_id_type=MESH,
            )
            copy.start()
            scatters.append(copy)

    scatters = []
    keep_copy.wait()

    def fresh(k, _):
        load(k).wait()

        @pl.when(k + DEPTH < blocks)
        def _():
            load(k + DEPTH).start()

        span = pl.ds(pl.multiple_of(k * block, block), block)
        mr = turned(span, 0)
        left = jnp.concatenate([mr, turned(span, half), turned(span, half + side)], 0)
        acc[:3 * side, :] += jnp.dot(left, x_buf[span, half:], preferred_element_type=jnp.float32)
        acc[3 * side:, :] += jnp.dot(mr, x_buf[span, :half], preferred_element_type=jnp.float32)
        return 0

    acc[...] = jnp.zeros_like(acc)
    late[...] = jnp.zeros_like(late)
    lax.fori_loop(0, blocks, fresh, 0)
    cr = acc[:side, :]
    re = acc[side:half, :] + acc[3 * side:, :]
    cross[...] = cr[:, side:]
    packed[:side, :side] = jnp.where(r <= c, re[:, :side], cr[:, :side].T - cr[:, :side])
    packed[:side, side:] = re[:, side:]
    trace = jnp.sum(jnp.where(r == c, re[:, :side], 0.0), axis=0, keepdims=True)
    pl.semaphore_wait(barrier, n + m - 2)
    early = chunks // 2
    for k in range(early):
        send(k)

    def again(k, _):
        span = pl.ds(pl.multiple_of(k * wide, wide), wide)
        late[...] += jnp.dot(turned(span, side), x_buf[span, :], preferred_element_type=jnp.float32)
        return 0

    wide = min(WIDE, cells)
    lax.fori_loop(0, cells // wide, again, 0)
    cr = late[:, half:]
    re = acc[half:half + side, side:] + late[:, side:half]
    packed[side:, :side] = cross[...].T - cr[:, :side]
    packed[side:, side:] = jnp.where(r <= c, re, cr[:, side:].T - cr[:, side:])
    trace = trace + jnp.sum(jnp.where(r == c, re, 0.0), axis=0, keepdims=True)
    tr_src[...] = trace
    traces = []
    for k in range(1, m):
        copy = pltpu.make_async_remote_copy(
            src_ref=tr_src,
            dst_ref=tr_buf.at[k - 1],
            send_sem=tr_send.at[k - 1],
            recv_sem=tr_recv.at[k - 1],
            device_id=(me, lax.rem(g + k, m)),
            device_id_type=MESH,
        )
        copy.start()
        traces.append(copy)
    for k in range(early, chunks):
        send(k)

    gathers = []
    for k in range(chunks):
        if k == chunks - 1:
            for copy in traces:
                copy.wait()
            power = tr_src[...]
            for j in range(m - 1):
                power = power + tr_buf[j]
            both = jnp.concatenate([power, tr_src[...]], 0)
            pw_src[...] = both
            pw_ref[me] = both
            spread = []
            for j in range(1, n):
                copy = pltpu.make_async_remote_copy(
                    src_ref=pw_src,
                    dst_ref=pw_ref.at[me],
                    send_sem=pw_send.at[j - 1],
                    recv_sem=pw_recv.at[j - 1],
                    device_id=(lax.rem(me + j, n), g),
                    device_id_type=MESH,
                )
                copy.start()
                spread.append(copy)
        for copy in scatters[k * (n - 1):(k + 1) * (n - 1)]:
            copy.wait()
        total = packed[pl.ds(pl.multiple_of((k * n + me) * rows, rows), rows), :]
        for j in range(n - 1):
            total = total + rs_buf[k, j]
        mine[k] = total
        out_ref[k, me] = total
        for j in range(1, n):
            copy = pltpu.make_async_remote_copy(
                src_ref=mine.at[k],
                dst_ref=out_ref.at[k, me],
                send_sem=ag_send.at[k, j - 1],
                recv_sem=ag_recv.at[k, j - 1],
                device_id=(lax.rem(me + j, n), g),
                device_id_type=MESH,
            )
            copy.start()
            gathers.append((k, j, copy))
    for j in range(1, n):
        spread[j - 1].wait_send()
        peer = lax.rem(me + n - j, n)
        pltpu.make_async_remote_copy(
            src_ref=pw_src,
            dst_ref=pw_ref.at[peer],
            send_sem=pw_send.at[j - 1],
            recv_sem=pw_recv.at[j - 1],
            device_id=(peer, g),
            device_id_type=MESH,
        ).wait_recv()
    for k, j, copy in gathers:
        copy.wait_send()
        peer = lax.rem(me + n - j, n)
        pltpu.make_async_remote_copy(
            src_ref=mine.at[k],
            dst_ref=out_ref.at[k, peer],
            send_sem=ag_send.at[k, j - 1],
            recv_sem=ag_recv.at[k, j - 1],
            device_id=(peer, g),
            device_id_type=MESH,
        ).wait_recv()


def gram_sum(snaps, keep):
    n, m = lax.axis_size("cells"), lax.axis_size("bins")
    cells, width = snaps.shape
    half = width // 2
    side = half // 2
    chunks = max(1, min(CHUNKS, half // (8 * n)))
    rows = half // (n * chunks)
    blocks = max(1, cells // BLOCK)
    dma = pltpu.SemaphoreType.DMA
    f32, vmem = jnp.float32, pltpu.VMEM
    return pl.pallas_call(
        functools.partial(sum_kernel, n, m, chunks, blocks),
        out_shape=(
            jax.ShapeDtypeStruct((chunks, n, rows, half), f32),
            jax.ShapeDtypeStruct((n, 2, side), f32),
        ),
        in_specs=[pl.BlockSpec(memory_space=pltpu.HBM)] * 2,
        out_specs=(pl.BlockSpec(memory_space=pltpu.VMEM),) * 2,
        scratch_shapes=[
            vmem((1, cells), jnp.int32),
            vmem((cells, width), jnp.bfloat16),
            vmem((4 * side, half), f32),
            vmem((side, width), f32),
            vmem((side, side), f32),
            vmem((half, half), f32),
            vmem((chunks, n - 1, rows, half), f32),
            vmem((1, side), f32),
            vmem((m - 1, 1, side), f32),
            vmem((2, side), f32),
            vmem((chunks, rows, half), f32),
            dma(()),
            dma((blocks,)),
            [dma((chunks, n - 1)), dma((chunks, n - 1)), dma((m - 1,)), dma((m - 1,)), dma((n - 1,)), dma((n - 1,)), dma((chunks, n - 1)), dma((chunks, n - 1))],
        ],
        compiler_params=pltpu.CompilerParams(
            collective_id=0, has_side_effects=True, vmem_limit_bytes=VMEM_LIMIT
        ),
        name="gram_sum",
    )(keep, snaps)


def grow(d):
    return (4.0 * d - 2.0 * d * d) / (1.0 + 2.0 * d - d * d)


def start_for(steps, goal):
    lo, hi = 0.0, 1.0
    for _ in range(100):
        mid = 0.5 * (lo + hi)
        d = mid
        for _ in range(steps):
            d = grow(d)
        lo, hi = (lo, mid) if d >= goal else (mid, hi)
    return hi


def split(x, parts):
    out = []
    for _ in range(parts):
        top = x.astype(jnp.bfloat16)
        out.append(top)
        x = x - top.astype(jnp.float32)
    return out


def mxu(a, b):
    return jnp.dot(a, b, preferred_element_type=jnp.float32)


def total(x):
    return jnp.sum(jnp.sum(x, axis=0, keepdims=True), axis=1, keepdims=True)


def steer_rows(doppler, chans, pulses):
    bins, dim = doppler.shape[1], chans * pulses
    at = lax.broadcasted_iota(jnp.int32, (bins, bins), 0)
    to = lax.broadcasted_iota(jnp.int32, (bins, bins), 1)
    doppler = jnp.sum(
        jnp.where(at == to, doppler.astype(jnp.float32), 0.0), axis=1, keepdims=True
    )
    index = lax.broadcasted_iota(jnp.int32, (1, dim), 1)
    pulse = lax.rem(index, pulses)
    chan = ((index - pulse) // pulses).astype(jnp.float32)
    freq = doppler * (1.0 / NDOPP) - 0.5
    turns = look_freq * chan + pulse.astype(jnp.float32) * freq
    phase = (2.0 * math.pi) * turns
    quarter = jnp.floor(4.0 * turns + 0.5)
    rest = phase - quarter * 1.5703125
    rest = rest - quarter * 4.837512969970703125e-4
    rest = rest - quarter * 7.549789948768648e-8
    sq = rest * rest
    sin = rest + rest * sq * (
        -1.6666654611e-1 + sq * (8.3321608736e-3 + sq * -1.9515295891e-4)
    )
    cos = 1.0 + sq * (
        -0.5 + sq * (4.166664568298827e-2 + sq * (-1.388731625493765e-3 + sq * 2.443315711809948e-5))
    )
    which = quarter.astype(jnp.int32) & 3
    odd = (which & 1) == 1
    c = jnp.where(odd, sin, cos)
    s = jnp.where(odd, cos, sin)
    c = jnp.where((which == 1) | (which == 2), -c, c)
    s = jnp.where(which >= 2, -s, s)
    return jnp.concatenate([c, s], 1) * (1.0 / math.sqrt(dim))


def solve_kernel(
    groups, block, sum_ref, pw_ref, dop_hbm, x_hbm, out_hbm,
    dop, x_buf, out_buf, taps, re_parts, im_parts, pair, wide, xs, ys, acol, steer, w_ref,
    dop_sem, in_sems, out_sems,
):
    half = sum_ref.shape[0]
    full = 2 * half
    bins = dop.shape[1]
    cells = x_buf.shape[0]
    f32, bf16 = jnp.float32, jnp.bfloat16

    dop_copy = pltpu.make_async_copy(dop_hbm, dop, dop_sem)
    dop_copy.start()
    loads = []
    for k in range(cells // block):
        span = pl.ds(k * block, block)
        copy = pltpu.make_async_copy(x_hbm.at[span], x_buf.at[span], in_sems.at[k])
        copy.start()
        loads.append(copy)

    power = pw_ref[0]
    for k in range(1, pw_ref.shape[0]):
        power = power + pw_ref[k]
    power = jnp.sum(power, axis=1, keepdims=True)
    low = (load_ratio / (groups * half)) * power[:1]
    bound = 1.0001 * power[1:]
    scale = 2.0 / (bound + 2.0 * low)
    side = half // 2
    r = lax.broadcasted_iota(jnp.int32, (side, side), 0)
    c = lax.broadcasted_iota(jnp.int32, (side, side), 1)
    eye = jnp.where(r == c, 1.0, 0.0)

    def put(i, j, xr, xi):
        at, to = slice(i * side, (i + 1) * side), slice(j * side, (j + 1) * side)
        acol[at, to] = xr
        acol[half + i * side:half + (i + 1) * side, to] = xi
        for k, (tr, ti) in enumerate(zip(split(xr, 3), split(xi, 3))):
            re_parts[k * half + i * side:k * half + (i + 1) * side, to] = tr
            im_parts[k * half + i * side:k * half + (i + 1) * side, to] = ti
            if k == 0:
                pair[at, to] = tr
                pair[half + i * side:half + (i + 1) * side, to] = ti

    for i in range(2):
        own = sum_ref[i * side:(i + 1) * side, i * side:(i + 1) * side]
        flip = own.T
        xr = (jnp.where(r <= c, own, flip) + low * eye) * scale
        xi = jnp.where(r > c, own, jnp.where(r < c, -flip, 0.0)) * scale
        put(i, i, xr, xi)
    upper = sum_ref[:side, side:] * scale
    lower = sum_ref[side:, :side] * scale
    put(0, 1, upper, -lower.T)
    put(1, 0, upper.T, lower)

    def times(left, re, im):
        rows = left.shape[0] // 2
        p, q = mxu(left, re), mxu(left, im)
        return p[:rows] - q[rows:], p[rows:] + q[:rows]

    square = jnp.concatenate(times(pair[:full, :], re_parts[:half, :], im_parts[:half, :]), 0)
    top = total(square * square)
    dop_copy.wait()
    steer[...] = steer_rows(dop[...], CHANNELS, PULSES)

    lam = 1.005 * jnp.sqrt(jnp.sqrt(top)) / scale - low
    tight = jnp.minimum(bound, jnp.maximum(lam, 0.0))
    gainup = (bound + 2.0 * low) / (tight + 2.0 * low)
    d0 = 2.0 * low / (tight + 2.0 * low)

    def bend_of(d):
        return 2.0 / (1.0 + 2.0 * d - d * d)

    def pack(at, v):
        pair[at * half:at * half + full, :] = v.astype(bf16)

    def first(square, d):
        bend = bend_of(d)
        a = acol[...] * (bend * gainup)
        x1 = -a
        xs[...] = x1
        for i in range(2):
            at = slice(i * side, (i + 1) * side)
            xs[at, at] = x1[at, at] + (2.0 * bend) * eye
        ys[...] = 2.0 * a - square * (bend * gainup * gainup)
        return grow(d)

    def steps_of(d):
        count = jnp.zeros_like(d)
        for k in range(2, 12):
            count = count + jnp.where(d < START[k], 1.0, 0.0)
        return jnp.max(count).astype(jnp.int32)

    coarse = jnp.max(jnp.where(d0 < COARSE, 1.0, 0.0)) > 0.5

    @pl.when(jnp.logical_not(coarse))
    def _():
        d1 = first(square, d0)
        pack(0, xs[...])
        pack(2, ys[...])

        def body(_, d):
            bend = bend_of(d)
            p = mxu(pair[...], pair[full:full + half, :])
            q = mxu(pair[...], pair[full + half:, :])
            for at, ref in ((0, xs), (full, ys)):
                re = bend * (2.0 * ref[:half, :] - (p[at:at + half] - q[at + half:at + full]))
                im = bend * (2.0 * ref[half:, :] - (p[at + half:at + full] + q[at:at + half]))
                ref[:half, :] = re
                ref[half:, :] = im
                pair[at:at + half, :] = re.astype(bf16)
                pair[at + half:at + full, :] = im.astype(bf16)
            return grow(d)

        d = lax.fori_loop(0, steps_of(d0), body, d1)
        bend = bend_of(d)
        re, im = times(pair[:full, :], pair[full:full + half, :], pair[full + half:, :])
        pair[:half, :] = (bend * (2.0 * xs[:half, :] - re)).astype(bf16)
        pair[half:full, :] = (bend * (2.0 * xs[half:, :] - im)).astype(bf16)

    @pl.when(coarse)
    def _():
        def product(left, ref):
            wide[:half, :half] = left[:half]
            wide[half:, half:] = left[:half]
            wide[:half, half:] = -left[half:]
            wide[half:, :half] = left[half:]
            return jnp.dot(wide[...], ref[...], preferred_element_type=f32, precision=HIGH)

        d1 = first(product(acol[...], acol), d0)

        def body(_, d):
            bend = bend_of(d)
            xs[...] = bend * (2.0 * xs[...] - product(xs[...], ys))
            ys[...] = bend * (2.0 * ys[...] - product(ys[...], ys))
            return grow(d)

        lax.fori_loop(0, steps_of(d0) + 1, body, d1)
        pack(0, xs[...])

    def stack(v):
        return jnp.concatenate([v[:, :half], v[:, half:]], 0).astype(bf16)

    def apply(v):
        left = stack(v)
        p, q = mxu(left, pair[:half, :]), mxu(left, pair[half:full, :])
        return jnp.concatenate([p[:bins] + q[bins:], p[bins:] - q[:bins]], 1) * gainup

    def short(v):
        return v.astype(bf16).astype(f32)

    def less(rest, w, parts):
        left = jnp.concatenate([stack(w)] * parts, 1)
        p = mxu(left, re_parts[:parts * half, :])
        q = mxu(left, im_parts[:parts * half, :])
        return rest - jnp.concatenate([p[:bins] + q[bins:], p[bins:] - q[:bins]], 1)

    w0 = short(apply(steer[...]))
    rest = less(steer[...], w0, 3)
    w1 = short(apply(rest))
    rest = less(rest, w1, 3)
    w2 = short(apply(rest))
    rest = less(rest, w2, 2)
    w_ref[...] = w0 + (w1 + (w2 + apply(rest)))

    @pl.when(coarse)
    def _():
        def body(_, w):
            rest = steer[...]
            for part in split(w, 3):
                rest = less(rest, part.astype(f32), 3)
            return w + apply(rest)
        w_ref[...] = lax.fori_loop(0, 4, body, w_ref[...])

    w = w_ref[...]
    gain = jnp.sum(steer[...] * w, axis=1, keepdims=True)
    w = w / gain
    wr, wi = w[:, :half], w[:, half:]
    taps[:bins, :half] = wr.astype(bf16)
    taps[:bins, half:] = wi.astype(bf16)
    taps[bins:, :half] = (-wi).astype(bf16)
    taps[bins:, half:] = wr.astype(bf16)

    for copy in loads:
        copy.wait()
    stores = []
    for k in range(cells // block):
        span = pl.ds(k * block, block)
        out_buf[:, span] = lax.dot_general(
            taps[...], x_buf[span, :], (((1,), (1,)), ((), ())), preferred_element_type=f32
        ).astype(bf16)
        copy = pltpu.make_async_copy(out_buf.at[:, span], out_hbm.at[:, span], out_sems.at[k])
        copy.start()
        stores.append(copy)
    for copy in stores:
        copy.wait()


GOAL = 0.95
START = [start_for(k, GOAL) for k in range(12)]
COARSE = 0.005
CHUNKS = 2
DEPTH = 2
BLOCK = 2048
WIDE = 2048
VMEM_LIMIT = 52 * 1024 * 1024


def solve(summed, power, doppler, snaps, groups, block):
    half = summed.shape[0]
    bins = doppler.shape[1]
    cells, width = snaps.shape
    full = 2 * half
    f32, bf16 = jnp.float32, jnp.bfloat16
    vmem = pltpu.VMEM
    dma = pltpu.SemaphoreType.DMA
    return pl.pallas_call(
        functools.partial(solve_kernel, groups, block),
        out_shape=jax.ShapeDtypeStruct((2 * bins, cells), bf16),
        in_specs=[
            pl.BlockSpec(memory_space=pltpu.VMEM),
            pl.BlockSpec(memory_space=pltpu.VMEM),
            pl.BlockSpec(memory_space=pltpu.HBM),
            pl.BlockSpec(memory_space=pltpu.HBM),
        ],
        out_specs=pl.BlockSpec(memory_space=pltpu.HBM),
        scratch_shapes=[
            vmem((1, bins), jnp.int32),
            vmem((cells, width), bf16),
            vmem((2 * bins, cells), bf16),
            vmem((2 * bins, width), bf16),
            vmem((3 * half, half), bf16),
            vmem((3 * half, half), bf16),
            vmem((2 * full, half), bf16),
            vmem((full, full), f32),
            vmem((full, half), f32),
            vmem((full, half), f32),
            vmem((full, half), f32),
            vmem((bins, full), f32),
            vmem((bins, full), f32),
            dma(()),
            dma((cells // block,)),
            dma((cells // block,)),
        ],
        compiler_params=pltpu.CompilerParams(vmem_limit_bytes=VMEM_LIMIT),
        name="solve",
    )(summed, power, doppler, snaps)


def per_device(snapshots, training, doppler):
    snaps = snapshots[0]
    keep = pltpu.with_memory_space_constraint(training[None, :], pltpu.HBM)
    parts, power = gram_sum(snaps, keep)
    half = parts.shape[3]
    summed = parts.reshape(half, half)
    return solve(summed, power, doppler, snaps, lax.axis_size("bins"), 1024)[None]


def solution(mesh):
    in_specs = (P("bins", "cells", None), P("cells"), P("bins", None))
    out_specs = P("bins", None, "cells")
    return jax.shard_map(
        per_device, mesh=mesh, in_specs=in_specs, out_specs=out_specs, check_vma=False
    )
```
